256 devices in a mesh: rows: 16 (over z_lo, x), cols: 16 (over y, z_hi, core).
Axes of the slice: x: 4, y: 4, z: 8 (z_hi: 2, z_lo: 4; z = z_hi * 4 + z_lo), core: 2. Of those that a mesh axis runs over, the one named last changes fastest.
Arguments:
- kernel_hat: bfloat16 [2, 256, 512, 4096], P(None, 'rows', 'cols'), may hold values from -0.5 to 0.5
- coefficients: float32 [128, 512], P(None, 'cols'), may hold values from -6 to 6
- wave_speed_sq: float32 [4096, 4096], P('rows', 'cols'), may hold values from 1 to 4
- wet_mask: int32 [4096, 4096], P('rows', 'cols'), may hold values 0 or 1
- boundary_cell: int32 [4096], replicated, may hold values from 0 to 4095, each once
- height: float32 [4096, 4096], P('rows', 'cols'), may hold values from -3 to 3
- flux_x: float32 [4096, 4096], P('rows', 'cols'), may hold values from -3 to 3
- flux_y: float32 [4096, 4096], P('rows', 'cols'), may hold values from -3 to 3
Outputs:
- boundary_series: float32 [128, 4096], P('rows', 'cols')
- height_out: float32 [4096, 4096], P('rows', 'cols')
- flux_x_out: float32 [4096, 4096], P('rows', 'cols')
- flux_y_out: float32 [4096, 4096], P('rows', 'cols')
The draws below stay inside these ranges and needn't reach their ends.
Inputs may be any that keep to these rules, and one draw needn't show every extreme that they name: `boundary_cell`: each of the 4096 boundary points names a different grid column, so each column is named by exactly one point.
All inputs are finite; a program needn't handle non-finite values. No bound on the sum of `wet_mask` on one device may be relied on, other than what follows from the above.
Results may differ from the reference program's by a relative error of at most 0.0029.
Values sent between devices are 32-bit elements; how exact they have to be, the bound alone decides.
No kernel may reach another device: no remote copies, remote signals or barrier semaphores. Data moves between devices by JAX's collectives and lax.ppermute only.
A program may use at most 64 MiB of HBM per device.

```python
import math
import jax
import jax.numpy as jnp
from jax import lax

NT = 128
SRC = 512
NF = 256
OBS = 4096
NR = 4096
NC = 4096


def touch_ends(array, own_key, least, top_value):
    longest = array.shape.index(max(array.shape))
    spots = []
    for shift in (0, 1):
        where = [jax.random.randint(jax.random.fold_in(own_key, axis), (), 0, length) for axis, length in enumerate(array.shape)]
        where[longest] = (where[longest] + shift) % array.shape[longest]
        spots.append(tuple(where))
    return array.at[spots[0]].set(least).at[spots[1]].set(top_value)


def block_scale(rng, extent, shards, least, largest):
    factor_of, own = 1.0, jax.random.fold_in(rng, 6)
    for axis_at, shards_of in shards:
        steps = jnp.exp(jax.random.uniform(jax.random.fold_in(own, axis_at), (shards_of,), jnp.float32, least / len(shards), largest / len(shards)))
        factor_of = factor_of * jnp.repeat(steps, extent[axis_at] // shards_of).reshape([-1 if axis == axis_at else 1 for axis in range(len(extent))])
    return factor_of


def scatter_about(key, shape, width, reach, cuts=(), kind=jnp.bfloat16):
    values = width * jax.random.normal(key, shape, jnp.float32)
    if cuts:
        values = values * block_scale(key, shape, cuts, -0.22, 0.18)
    return jnp.clip(values, -reach, reach).astype(kind)


def setup_inputs(seed: int = 0) -> dict:
    keys = jax.random.split(jax.random.key(seed), 9)
    return {
        "kernel_hat": scatter_about(keys[0], (2, NF, SRC, OBS), (SRC // 4) ** -0.5, 0.5, ((1, 16), (2, 16))),
        "coefficients": scatter_about(keys[1], (NT, SRC), 1.0, 6.0, ((1, 16),), jnp.float32),
        "wave_speed_sq": jnp.clip(jnp.exp(math.log(4.0) - 1.3862944 * jax.random.uniform(keys[2], (NR, NC), jnp.float32) ** block_scale(keys[2], (NR, NC), ((0, 16), (1, 16)), -0.2, 0.2)), 1.0, 4.0),
        "wet_mask": touch_ends((jax.random.randint(keys[3], (NR, NC), 0, 4) < 3).astype(jnp.int32), jax.random.fold_in(keys[3], 1), 0, 1),
        "boundary_cell": jax.random.permutation(keys[4], OBS).astype(jnp.int32),
        "height": scatter_about(keys[5], (NR, NC), 0.5, 3.0, ((0, 16), (1, 16)), jnp.float32),
        "flux_x": scatter_about(keys[6], (NR, NC), 0.5, 3.0, ((0, 16), (1, 16)), jnp.float32),
        "flux_y": scatter_about(keys[7], (NR, NC), 0.5, 3.0, ((0, 16), (1, 16)), jnp.float32),
    }


STEP_RATIO = 0.25

def neighbours(values, along_dim):
    if along_dim == 1:
        return (values[1:-1, :-1], values[1:-1, 1:])
    return (values[:-1, 1:-1], values[1:, 1:-1])

def face_fluxes(surface, along, across, speed_sq, celerity, wet, along_dim):
    left_surf, right_surf = neighbours(surface, along_dim)
    left_along, right_along = neighbours(along, along_dim)
    left_across, right_across = neighbours(across, along_dim)
    left_sq, right_sq = neighbours(speed_sq, along_dim)
    left_speed, right_speed = neighbours(celerity, along_dim)
    left_wet, right_wet = neighbours(wet, along_dim)
    opened = left_wet * right_wet
    damping = 0.25 * (left_speed + right_speed)
    mass_flux = opened * (0.5 * (left_along + right_along) - damping * (right_surf - left_surf))
    momentum = opened * (0.5 * (left_sq * left_surf + right_sq * right_surf) - damping * (right_along - left_along))
    shear_flux = opened * (-damping * (right_across - left_across))
    return (mass_flux, momentum, shear_flux)

def advance(surface, along_x, along_y, speed_sq, wet):
    celerity = jnp.sqrt(speed_sq)
    mass_x, momentum_x, shear_x = face_fluxes(surface, along_x, along_y, speed_sq, celerity, wet, 1)
    mass_y, momentum_y, shear_y = face_fluxes(surface, along_y, along_x, speed_sq, celerity, wet, 0)
    interior_wet = wet[1:-1, 1:-1]

    def update(values, flux_cols, flux_rows):
        change = flux_cols[:, 1:] - flux_cols[:, :-1] + (flux_rows[1:] - flux_rows[:-1])
        return interior_wet * (values[1:-1, 1:-1] - STEP_RATIO * change)
    return (update(surface, mass_x, mass_y), update(along_x, momentum_x, shear_y), update(along_y, shear_x, momentum_y))

def reference(kernel_hat, coefficients, wave_speed_sq, wet_mask, boundary_cell, height, flux_x, flux_y):
    spectrum = jnp.fft.fft(coefficients, n=NF, axis=0)
    coef_re = lax.optimization_barrier(jnp.real(spectrum).astype(jnp.bfloat16)).astype(jnp.float32)
    coef_im = lax.optimization_barrier(jnp.imag(spectrum).astype(jnp.bfloat16)).astype(jnp.float32)
    high = lax.Precision.HIGHEST

    def one_frequency(index):
        kern_re = lax.dynamic_index_in_dim(kernel_hat[0], index, 0, keepdims=False).astype(jnp.float32)
        kern_im = lax.dynamic_index_in_dim(kernel_hat[1], index, 0, keepdims=False).astype(jnp.float32)
        row_re = lax.dynamic_index_in_dim(coef_re, index, 0, keepdims=False)
        row_im = lax.dynamic_index_in_dim(coef_im, index, 0, keepdims=False)
        spec_re = jnp.dot(row_re, kern_re, precision=high) - jnp.dot(row_im, kern_im, precision=high)
        spec_im = jnp.dot(row_im, kern_re, precision=high) + jnp.dot(row_re, kern_im, precision=high)
        return (spec_re, spec_im)
    spec_re, spec_im = lax.map(one_frequency, jnp.arange(NF, dtype=jnp.int32))
    times = jnp.arange(NT, dtype=jnp.int32)
    freqs = jnp.arange(NF, dtype=jnp.int32)
    phase = (times[:, None] * freqs[None, :] % NF).astype(jnp.float32) * (2.0 * math.pi / NF)
    series = (jnp.dot(jnp.cos(phase), spec_re, precision=high) - jnp.dot(jnp.sin(phase), spec_im, precision=high)) / NF
    latest = series[NT - 2:]
    ghost = jnp.zeros((2, NC), jnp.float32).at[:, boundary_cell].set(latest)
    wet = wet_mask.astype(jnp.float32)
    speed_pad = jnp.pad(wave_speed_sq, 1).at[-1].set(1.0)
    wet_pad = jnp.pad(wet, 1).at[-1].set(1.0)
    surface, along_x, along_y = (height, flux_x, flux_y)
    for step in range(2):
        surf_pad = jnp.pad(surface, 1).at[-1, 1:-1].set(ghost[step])
        surface, along_x, along_y = advance(surf_pad, jnp.pad(along_x, 1), jnp.pad(along_y, 1), speed_pad, wet_pad)
    return (series, surface, along_x, along_y)
```

```python
import math

import jax
import jax.numpy as jnp
from jax import lax
from jax.sharding import PartitionSpec as P

STEP_RATIO = 0.25
HIGH = lax.Precision.HIGHEST
SIDE = 16
FREQ_DEV = 16
PAIRS = [(i, i ^ 1) for i in range(SIDE)]
ODD_PAIRS = [(i, i + 1) for i in range(1, SIDE - 1, 2)] + [(i + 1, i) for i in range(1, SIDE - 1, 2)]


def swap(x, axis, bits):
    return lax.ppermute(x, axis, [(i, i ^ bits) for i in range(SIDE)])


def pick(x, index):
    return lax.dynamic_index_in_dim(x, index, 0, keepdims=False)


def neighbours(values, along_dim):
    if along_dim == 1:
        return (values[1:-1, :-1], values[1:-1, 1:])
    return (values[:-1, 1:-1], values[1:, 1:-1])


def face_fluxes(surface, along, across, speed_sq, celerity, wet, along_dim):
    left_surf, right_surf = neighbours(surface, along_dim)
    left_along, right_along = neighbours(along, along_dim)
    left_across, right_across = neighbours(across, along_dim)
    left_sq, right_sq = neighbours(speed_sq, along_dim)
    left_speed, right_speed = neighbours(celerity, along_dim)
    left_wet, right_wet = neighbours(wet, along_dim)
    opened = left_wet * right_wet
    damping = 0.25 * (left_speed + right_speed)
    mass_flux = opened * (0.5 * (left_along + right_along) - damping * (right_surf - left_surf))
    momentum = opened * (
        0.5 * (left_sq * left_surf + right_sq * right_surf) - damping * (right_along - left_along)
    )
    shear_flux = opened * (-damping * (right_across - left_across))
    return (mass_flux, momentum, shear_flux)


def advance(surface, along_x, along_y, speed_sq, wet):
    celerity = jnp.sqrt(speed_sq)
    mass_x, momentum_x, shear_x = face_fluxes(surface, along_x, along_y, speed_sq, celerity, wet, 1)
    mass_y, momentum_y, shear_y = face_fluxes(surface, along_y, along_x, speed_sq, celerity, wet, 0)
    interior_wet = wet[1:-1, 1:-1]

    def update(values, flux_cols, flux_rows):
        change = flux_cols[:, 1:] - flux_cols[:, :-1] + (flux_rows[1:] - flux_rows[:-1])
        return interior_wet * (values[1:-1, 1:-1] - STEP_RATIO * change)

    return (
        update(surface, mass_x, mass_y),
        update(along_x, momentum_x, shear_y),
        update(along_y, shear_x, momentum_y),
    )


def spectrum(kernel_hat, coefficients, freqs, times, freq_total):
    factor = 2.0 * math.pi / freq_total
    forward = (freqs[:, None] * times[None, :] % freq_total).astype(jnp.float32) * factor
    coef_re = jnp.dot(jnp.cos(forward), coefficients, precision=HIGH).astype(jnp.bfloat16)
    coef_im = (-jnp.dot(jnp.sin(forward), coefficients, precision=HIGH)).astype(jnp.bfloat16)
    form = "fso,fs->fo"
    kern_re, kern_im = kernel_hat[0], kernel_hat[1]
    spec_re = jnp.einsum(form, kern_re, coef_re, preferred_element_type=jnp.float32) - jnp.einsum(
        form, kern_im, coef_im, preferred_element_type=jnp.float32
    )
    spec_im = jnp.einsum(form, kern_re, coef_im, preferred_element_type=jnp.float32) + jnp.einsum(
        form, kern_im, coef_re, preferred_element_type=jnp.float32
    )
    return jnp.concatenate([spec_re, spec_im], axis=0)


def ghost_tiles(part, table, boundary_cell):
    last = jnp.dot(table[-2:], part, precision=HIGH)
    high_of = boundary_cell // 128
    low_of = boundary_cell % 128
    in_high = (high_of[None, :] == jnp.arange(32, dtype=jnp.int32)[:, None]).astype(jnp.float32)
    in_low = (low_of[None, :] == jnp.arange(128, dtype=jnp.int32)[:, None]).astype(jnp.float32)
    spread = (last[:, None, :] * in_high[None]).reshape(64, -1)
    placed = lax.dot_general(spread, in_low, (((1,), (1,)), ((), ())), precision=HIGH)
    first, second = placed[:32], placed[32:]
    nothing = jnp.zeros((1, 128), jnp.float32)
    before = jnp.concatenate([nothing, first[1:-1:2]], axis=0)
    after = jnp.concatenate([first[2::2], nothing], axis=0)
    return jnp.concatenate(
        [
            first.reshape(SIDE, 2, 128),
            second.reshape(SIDE, 2, 128),
            before[:, None],
            after[:, None],
            jnp.zeros((SIDE, 2, 128), jnp.float32),
        ],
        axis=1,
    )


def halo_rows(fields, index, axis):
    head, tail = fields[:, :2], fields[:, -2:]
    even = index % 2 == 0
    from_pair = lax.ppermute(jnp.where(even, tail, head), axis, PAIRS)
    from_other = lax.ppermute(jnp.where(even, head, tail), axis, ODD_PAIRS)
    return jnp.where(even, from_other, from_pair), jnp.where(even, from_pair, from_other)


def on_device(
    kernel_hat, coefficients, wave_speed_sq, wet_mask, boundary_cell, height, flux_x, flux_y
):
    row = lax.axis_index("rows")
    col = lax.axis_index("cols")
    core, z_hi, y = col % 2, (col // 2) % 2, col // 4
    freq_dev = kernel_hat.shape[1]
    steps_total = coefficients.shape[0]
    freq_total = freq_dev * SIDE
    freqs = row * freq_dev + jnp.arange(freq_dev, dtype=jnp.int32)
    times = jnp.arange(steps_total, dtype=jnp.int32)
    part = spectrum(kernel_hat, coefficients, freqs, times, freq_total)
    inverse = (times[:, None] * freqs[None, :] % freq_total).astype(jnp.float32) * (
        2.0 * math.pi / freq_total
    )
    table = jnp.concatenate([jnp.cos(inverse), -jnp.sin(inverse)], axis=1) / freq_total
    ghosts = ghost_tiles(part, table, boundary_cell)
    slots = part.reshape(32, SIDE, 2, 128).transpose(1, 2, 0, 3).reshape(SIDE, 64, 128)
    slots = jnp.concatenate([slots, ghosts], axis=1).reshape(8, 2, 72, 128)

    fields = jnp.stack([height, flux_x, flux_y, wave_speed_sq, wet_mask.astype(jnp.float32)])
    above, below = halo_rows(fields, row, "rows")
    tall = jnp.concatenate([above, fields, below], axis=1)
    left, right = halo_rows(jnp.swapaxes(jnp.concatenate([tall[:, :, :2], tall[:, :, -2:]], axis=2), 1, 2), col, "cols")
    padded = jnp.concatenate([jnp.swapaxes(left, 1, 2), tall, jnp.swapaxes(right, 1, 2)], axis=2)

    mine = lax.dynamic_index_in_dim(slots, core, 1, keepdims=False)
    other = lax.dynamic_index_in_dim(slots, 1 - core, 1, keepdims=False)
    block = (mine + swap(other, "cols", 1)).reshape(4, 2, 72, 128)
    got = [swap(pick(block, y ^ bits), "cols", 4 * bits) for bits in (1, 3, 2)]
    block = pick(block, y) + got[0] + got[1] + got[2]
    block = pick(block, z_hi) + swap(pick(block, 1 - z_hi), "cols", 2)

    spec = jnp.concatenate([block[:32], block[32:64]], axis=1)
    partial_value = jnp.dot(table, spec, precision=HIGH).reshape(SIDE, 8, 256)
    ghost = jnp.broadcast_to(block[64:][None], (SIDE, 8, 128))
    sent = jnp.concatenate([partial_value, ghost], axis=2)
    arrived = jnp.sum(lax.all_to_all(sent, "rows", 0, 0, tiled=True), axis=0)
    series, ghost = arrived[:, :256], arrived[:, 256:]

    surface, along_x, along_y, speed, wet = padded
    one = advance(surface, along_x, along_y, speed, wet)
    two = advance(*one, speed[1:-1, 1:-1], wet[1:-1, 1:-1])

    at_edge = row == SIDE - 1
    first = jnp.concatenate(
        [jnp.zeros((1, 1)), ghost[4:5, 127:], ghost[0:1], ghost[1:2], ghost[5:6, :1], jnp.zeros((1, 1))], axis=1
    )
    second = jnp.concatenate([ghost[4:5, 127:], ghost[2:3], ghost[3:4], ghost[5:6, :1]], axis=1)
    low = [x[-14:] for x in padded]
    ones = jnp.ones((1, 260), jnp.float32)
    last = jnp.zeros((1, 260), jnp.float32)
    edge = [
        jnp.concatenate([x[:-2], fill, last], axis=0) for x, fill in zip(low, (first, last, last, ones, ones))
    ]
    a, b, c = advance(*edge)
    a = jnp.concatenate([a[:-1], second], axis=0)
    b = jnp.concatenate([b[:-1], last[:, 2:]], axis=0)
    c = jnp.concatenate([c[:-1], last[:, 2:]], axis=0)
    edge = advance(a, b, c, edge[3][1:-1, 1:-1], edge[4][1:-1, 1:-1])
    result = [
        jnp.concatenate([x[:-8], jnp.where(at_edge, e[-8:], x[-8:])], axis=0) for x, e in zip(two, edge)
    ]
    return (series, *result)


def solution(mesh):
    return jax.shard_map(
        on_device,
        mesh=mesh,
        in_specs=(
            P(None, "rows", "cols", None),
            P(None, "cols"),
            P("rows", "cols"),
            P("rows", "cols"),
            P(),
            P("rows", "cols"),
            P("rows", "cols"),
            P("rows", "cols"),
        ),
        out_specs=(P("rows", "cols"), P("rows", "cols"), P("rows", "cols"), P("rows", "cols")),
        check_vma=False,
    )
```

```python
import math

import jax
import jax.numpy as jnp
from jax import lax
from jax.experimental import pallas as pl
from jax.experimental.pallas import tpu as pltpu
from jax.sharding import PartitionSpec as P


HIGH = lax.Precision.HIGHEST
SIDE = 16
PAIRS = [(i, i ^ 1) for i in range(SIDE)]
ODD_PAIRS = [(i, i + 1) for i in range(1, SIDE - 1, 2)] + [(i + 1, i) for i in range(1, SIDE - 1, 2)]
PAD = 16
TALL = 256 + 2 * PAD
WIDE = 384
VMEM = pl.BlockSpec(memory_space=pltpu.VMEM)
HBM = pl.BlockSpec(memory_space=pltpu.HBM)
F32 = jnp.float32


def like(*shape, dtype=F32):
    return jax.ShapeDtypeStruct(shape, dtype)


def params(limit=48):
    return pltpu.CompilerParams(vmem_limit_bytes=limit * 1024 * 1024)


def cost(flops, nbytes=1 << 16):
    return pl.CostEstimate(flops=flops, bytes_accessed=nbytes, transcendentals=0)


def swap(x, axis, bits):
    return lax.ppermute(x, axis, [(i, i ^ bits) for i in range(SIDE)])


def row_phase(rows, times, first, quarter):
    freq = first + 4 * (rows // 8) + rows % 4
    return (freq * times + quarter) & 255


def turn(phase):
    return jnp.cos(phase.astype(F32) * (2.0 * math.pi / 256))


def spectrum_kernel(chunks, kern_hbm, coef_ref, cell_ref, mine_ref, other_ref, data, last, low_hot, sems):
    wide = 4096 // chunks
    copies = []
    for n in range(chunks):
        part = pl.ds(n * wide, wide)
        copies.append(pltpu.make_async_copy(kern_hbm.at[:, :, :, part], data.at[n], sems.at[n]))
        copies[-1].start()
    even = lax.axis_index("cols") % 2 == 0
    first = lax.axis_index("rows") * 16

    rows = lax.broadcasted_iota(jnp.int32, (32, 128), 0)
    lanes = lax.broadcasted_iota(jnp.int32, (32, 128), 1)
    part_of = (rows // 4) % 2
    by_re = turn(row_phase(rows, lanes, first, 64 * part_of))
    by_im = turn(row_phase(rows, lanes, first, 64 * part_of - 64))
    coef = jnp.concatenate([coef_ref[...]] * 4, axis=0)
    contract = (((1,), (1,)), ((), ()))
    own = (lanes // 32) == (rows % 4)
    from_re = jnp.where(own, lax.dot_general(by_re, coef, contract, precision=HIGH, preferred_element_type=F32), 0.0)
    from_im = jnp.where(own, lax.dot_general(by_im, coef, contract, precision=HIGH, preferred_element_type=F32), 0.0)
    weights = jnp.concatenate([from_re, from_im], axis=1)
    weights = [weights[8 * g : 8 * g + 8].astype(jnp.bfloat16) for g in range(4)]

    cells = cell_ref[...]
    low_of, high_of = cells & 127, cells >> 7
    low_rows = lax.broadcasted_iota(jnp.int32, (128, 512), 0)
    for n in range(8):
        part = slice(n * 512, n * 512 + 512)
        low_hot[:, part] = jnp.where(low_of[:, part] == low_rows, 1.0, 0.0).astype(jnp.bfloat16)

    at_row = lax.broadcasted_iota(jnp.int32, (32, 1), 0)
    pair = [turn(row_phase(at_row, t, first, 64 * ((at_row // 4) % 2))) * (1.0 / 256) for t in (126, 127)]
    for n in range(chunks):
        copies[n].wait()
        got = []
        for g in range(4):
            rhs = jnp.concatenate(
                [data[n, p, 4 * g : 4 * g + 4].reshape(128, wide) for p in range(2)], axis=0
            )
            got.append(jnp.dot(weights[g], rhs, preferred_element_type=F32))
        value = jnp.concatenate(got, axis=0)
        for k in range(2):
            last[k : k + 1, n * wide : n * wide + wide] = jnp.sum(value * pair[k], axis=0, keepdims=True)
        for m in range(wide // 512):
            k = n * (wide // 512) + m
            for half in range(2):
                at = m * 512 + half * 128
                one, two = value[:, at : at + 128], value[:, at + 256 : at + 384]
                mine_ref[k, half * 32 : half * 32 + 32, :] = jnp.where(even, one, two)
                other_ref[k, half * 32 : half * 32 + 32, :] = jnp.where(even, two, one)

    high_rows = lax.broadcasted_iota(jnp.int32, (32, 512), 0)
    placed = jnp.zeros((128, 128), F32)
    for n in range(8):
        part = slice(n * 512, n * 512 + 512)
        here = high_of[:, part] == high_rows
        spread = []
        for k in range(2):
            value = last[k : k + 1, part]
            coarse = value.astype(jnp.bfloat16).astype(F32)
            for piece in (coarse, value - coarse):
                spread.append(jnp.where(here, piece, 0.0).astype(jnp.bfloat16))
        placed = placed + lax.dot_general(
            jnp.concatenate(spread, axis=0), low_hot[:, part], contract, preferred_element_type=F32
        )
    early = placed[0:32] + placed[32:64]
    late = placed[64:96] + placed[96:128]
    index = lax.broadcasted_iota(jnp.int32, (32, 128), 0)
    before = jnp.where(index == 0, 0.0, pltpu.roll(early, 1, 0))
    after = jnp.where(index == 30, 0.0, pltpu.roll(early, 30, 0))
    zeros = jnp.zeros((2, 128), F32)
    for k in range(8):
        tiles = []
        for c in range(2):
            j = 4 * k + 2 * c
            tiles.append(
                jnp.concatenate(
                    [early[j : j + 2], late[j : j + 2], before[j : j + 1], after[j : j + 1], zeros], axis=0
                )
            )
        mine_ref[k, 64:72, :] = jnp.where(even, tiles[0], tiles[1])
        other_ref[k, 64:72, :] = jnp.where(even, tiles[1], tiles[0])


def spectrum(kernel_hat, coefficients, boundary_cell):
    chunks = 8
    wide = 4096 // chunks

    def kernel(*refs):
        spectrum_kernel(chunks, *refs)

    return pl.pallas_call(
        kernel,
        out_shape=(like(8, 72, 128), like(8, 72, 128)),
        in_specs=[HBM, VMEM, VMEM],
        out_specs=(VMEM, VMEM),
        scratch_shapes=[
            pltpu.VMEM((chunks, 2, 16, 32, wide), jnp.bfloat16),
            pltpu.VMEM((8, 4096), F32),
            pltpu.VMEM((128, 4096), jnp.bfloat16),
            pltpu.SemaphoreType.DMA((chunks,)),
        ],
        compiler_params=params(),
        cost_estimate=cost(1 << 28, 8 << 20),
        name="spectrum",
    )(kernel_hat, coefficients.T, boundary_cell.reshape(1, -1))


def after_core_kernel(mine, got, keep, one, two, three):
    y = lax.axis_index("cols") // 4
    for out, bits in ((keep, 0), (one, 1), (two, 2), (three, 3)):
        at = pl.ds(2 * (y ^ bits), 2)
        out[...] = mine[at] + got[at]


def after_y_kernel(keep, one, two, three, mine, other):
    total = [keep[i] + one[i] + two[i] + three[i] for i in range(2)]
    low = (lax.axis_index("cols") // 2) % 2 == 0
    mine[...] = jnp.where(low, total[0], total[1])
    other[...] = jnp.where(low, total[1], total[0])


def after_z_kernel(mine, got, sent):
    first = lax.axis_index("rows") * 16
    times = lax.broadcasted_iota(jnp.int32, (128, 32), 0)
    at_row = lax.broadcasted_iota(jnp.int32, (128, 32), 1)
    table = turn(row_phase(at_row, times, first, 64 * ((at_row // 4) % 2))) * (1.0 / 256)
    block = mine[...] + got[...]
    spec = jnp.concatenate([block[:32], block[32:64]], axis=1)
    value = jnp.dot(table, spec, precision=HIGH, preferred_element_type=F32)
    for n in range(SIDE):
        sent[n, :, :256] = value[8 * n : 8 * n + 8]
        sent[n, :, 256:] = block[64:]


def whole(kernel, outs, flops, *args, scratch=()):
    return pl.pallas_call(
        kernel,
        out_shape=outs,
        in_specs=[VMEM] * len(args),
        out_specs=jax.tree.map(lambda _: VMEM, outs),
        scratch_shapes=scratch,
        compiler_params=params(),
        cost_estimate=cost(flops),
    )(*args)


def edge_rows_kernel(h, x, y, s, w, pair, other):
    even = lax.axis_index("rows") % 2 == 0
    pair[...] = jnp.zeros_like(pair)
    other[...] = jnp.zeros_like(other)
    for f, ref in enumerate((h, x, y, s, w)):
        head, tail = ref[0:2, :].astype(F32), ref[254:256, :].astype(F32)
        pair[2 * f : 2 * f + 2, :] = jnp.where(even, tail, head)
        other[2 * f : 2 * f + 2, :] = jnp.where(even, head, tail)


def sides(axis, pair, other):
    even = lax.axis_index(axis) % 2 == 0
    return jnp.where(even, other, pair), jnp.where(even, pair, other)


def edge_cols_kernel(h, x, y, s, w, row_pair, row_other, pair, other, mat):
    above, below = sides("rows", row_pair[...], row_other[...])
    mat[...] = jnp.zeros_like(mat)

    def place(rows, take):
        left_mix, lane = None, None
        for f in range(5):
            value = take(f)
            left = pltpu.roll(value[:, :128], 2 * f, 1) if f else value[:, :128]
            right = pltpu.roll(value[:, 128:], 18 + 2 * f, 1)
            if lane is None:
                lane = lax.broadcasted_iota(jnp.int32, left.shape, 1)
                left_mix = jnp.zeros(left.shape, F32)
            left_mix = jnp.where((lane // 2) == f, left, left_mix)
            left_mix = jnp.where((lane // 2) == 8 + f, right, left_mix)
        mat[rows, :] = left_mix

    for n in range(4):
        part = slice(64 * n, 64 * n + 64)
        place(slice(PAD + 64 * n, PAD + 64 * n + 64), lambda f: (h, x, y, s, w)[f][part, :].astype(F32))
    place(slice(PAD - 2, PAD), lambda f: above[2 * f : 2 * f + 2])
    place(slice(PAD + 256, PAD + 258), lambda f: below[2 * f : 2 * f + 2])
    even = lax.axis_index("cols") % 2 == 0
    for n in range(3):
        part = slice(128 * n, 128 * n + 128)
        flat = mat[part, :].T
        pair[:, part] = jnp.where(even, flat[16:32], flat[:16])
        other[:, part] = jnp.where(even, flat[:16], flat[16:32])


def right_of(v):
    return pltpu.roll(v, WIDE - 1, 1)


def left_of(v):
    return pltpu.roll(v, 1, 1)


def below_of(v):
    return pltpu.roll(v, v.shape[0] - 1, 0)


def above_of(v):
    return pltpu.roll(v, 1, 0)


def fluxes(after, h, q, p, e, c, w):
    opened = 0.5 * (w * after(w))
    damping = 0.5 * opened * (c + after(c))
    mass = opened * (q + after(q)) - damping * (after(h) - h)
    momentum = opened * (e + after(e)) - damping * (after(q) - q)
    shear = -damping * (after(p) - p)
    return mass, momentum, shear


def advance(h, x, y, s, c, w, top, rows):
    e = s * h
    mass_y, momentum_y, shear_y = fluxes(below_of, h, y, x, e, c, w)
    cut = lambda v: v[top : top + rows]
    rise = lambda v: cut(v - above_of(v))
    h, x, y, e, c, w = (cut(v) for v in (h, x, y, e, c, w))
    mass_x, momentum_x, shear_x = fluxes(right_of, h, x, y, e, c, w)
    step = lambda v, a, b: w * (v - 0.25 * ((a - left_of(a)) + rise(b)))
    return step(h, mass_x, mass_y), step(x, momentum_x, shear_y), step(y, shear_x, momentum_y)


def stencil_kernel(h, x, y, s, w, row_pair, row_other, col_pair, col_other, h_out, x_out, y_out, edge, fields, state):
    above, below = sides("rows", row_pair[...], row_other[...])
    left, right = sides("cols", col_pair[...], col_other[...])
    lane = lax.broadcasted_iota(jnp.int32, (WIDE, 128), 1)
    zeros = jnp.zeros((96, 128), F32)
    turned = jnp.concatenate(
        [
            jnp.concatenate([right[:, part], left[:, part], zeros], axis=0).T
            for part in (slice(0, 128), slice(128, 256), slice(256, 384))
        ],
        axis=0,
    )
    none = jnp.zeros((PAD, 256), F32)
    for f, ref in enumerate((h, x, y, s, w)):
        outer = pltpu.roll(turned, (128 - 2 * f) % 128, 1)
        inner = pltpu.roll(turned, 110 - 2 * f, 1)
        strip = jnp.where(lane < 2, outer, jnp.where(lane >= 126, inner, 0.0))[:TALL]
        fields[f, :, 256:] = strip
        fields[f, 0:PAD, :256] = none
        fields[f, PAD + 256 :, :256] = none
        fields[f, PAD - 2 : PAD, :256] = above[2 * f : 2 * f + 2]
        fields[f, PAD + 256 : PAD + 258, :256] = below[2 * f : 2 * f + 2]
        fields[f, PAD : PAD + 256, :256] = ref[...].astype(F32)
    for n in range(3):
        part = slice(96 * n, 96 * n + 96)
        fields[5, part, :] = jnp.sqrt(fields[3, part, :])

    size = 16
    for at in range(8, TALL - 8, size):
        part = slice(at - 8, at + size + 8)
        got = advance(*(fields[f, part, :] for f in (0, 1, 2, 3, 5, 4)), 8, size)
        for f in range(3):
            state[f, at : at + size, :] = got[f]
    for at in range(PAD, PAD + 256, size):
        part = slice(at - 8, at + size + 8)
        got = advance(*(state[f, part, :] for f in range(3)), *(fields[f, part, :] for f in (3, 5, 4)), 8, size)
        for f, out in enumerate((h_out, x_out, y_out)):
            out[at - PAD : at - PAD + size, :] = got[f][:, :256]
            if at == PAD + 256 - size:
                edge[6 + f, 0:8, :] = got[f][8:]
                edge[6 + f, 8:16, :] = jnp.zeros((8, WIDE), F32)
    for n, f in enumerate((0, 1, 2, 3, 5, 4)):
        edge[n] = fields[f, PAD + 248 : PAD + 264, :]


def last_kernel(arrived, edge, h_in, x_in, y_in, series, h_out, x_out, y_out):
    total = arrived[0]
    for n in range(1, SIDE):
        total = total + arrived[n]
    series[...] = total[:, :256]
    ghost = total[:, 256:]
    at_edge = lax.axis_index("rows") == SIDE - 1
    row = lax.broadcasted_iota(jnp.int32, (16, WIDE), 0)
    lane = lax.broadcasted_iota(jnp.int32, (1, 128), 1)
    first = jnp.concatenate(
        [ghost[0:1], ghost[1:2], jnp.where(lane == 0, ghost[5:6], jnp.where(lane == 127, ghost[4:5], 0.0))], axis=1
    )
    second = jnp.concatenate([ghost[2:3], ghost[3:4], jnp.zeros((1, 128), F32)], axis=1)
    beyond = row == 8
    h, x, y, s, c, w = (edge[n] for n in range(6))
    h, s, c, w = (jnp.where(beyond, fill, v) for v, fill in ((h, first), (s, 1.0), (c, 1.0), (w, 1.0)))
    x, y = (jnp.where(beyond, 0.0, v) for v in (x, y))
    h, x, y = advance(h, x, y, s, c, w, 0, 16)
    h, x, y = jnp.where(beyond, second, h), jnp.where(beyond, 0.0, x), jnp.where(beyond, 0.0, y)
    got = advance(h, x, y, s, c, w, 0, 16)
    redo = jnp.logical_and(at_edge, row[:8, :256] >= 6)
    for f, out in enumerate((h_out, x_out, y_out)):
        out[...] = jnp.where(redo, got[f][:8, :256], edge[6 + f, :8, :256])


def last_step(arrived, edge, height, flux_x, flux_y):
    grid_field = like(256, 256)
    row_block = pl.BlockSpec((8, 256), lambda i: (31, 0))
    return pl.pallas_call(
        last_kernel,
        grid=(1,),
        out_shape=(like(8, 256), grid_field, grid_field, grid_field),
        in_specs=[VMEM, VMEM, HBM, HBM, HBM],
        out_specs=(pl.BlockSpec((8, 256), lambda i: (0, 0)), row_block, row_block, row_block),
        input_output_aliases={2: 1, 3: 2, 4: 3},
        compiler_params=params(),
        cost_estimate=cost(1 << 20),
        name="last",
    )(arrived, edge, height, flux_x, flux_y)


def forecast(
    kernel_hat, coefficients, wave_speed_sq, wet_mask, boundary_cell, height, flux_x, flux_y
):
    fields = (height, flux_x, flux_y, wave_speed_sq, wet_mask)
    mine, other = spectrum(kernel_hat, coefficients, boundary_cell)
    got = swap(other, "cols", 1)
    slab = like(2, 72, 128)
    keep, one, two, three = whole(after_core_kernel, (slab,) * 4, 1 << 17, mine, got)
    got = [swap(v, "cols", bits) for v, bits in ((two, 8), (one, 4), (three, 12))]

    message = like(16, 256)
    pair, another = whole(edge_rows_kernel, (message, message), 1 << 14, *fields)
    row_pair = lax.ppermute(pair, "rows", PAIRS)
    row_other = lax.ppermute(another, "rows", ODD_PAIRS)

    slab = like(72, 128)
    mine, other = whole(after_y_kernel, (slab, slab), 1 << 17, keep, got[1], got[0], got[2])
    got = swap(other, "cols", 2)

    message = like(16, WIDE)
    scratch = [pltpu.VMEM((WIDE, 128), F32)]
    pair, another = whole(edge_cols_kernel, (message, message), 1 << 20, *fields, row_pair, row_other, scratch=scratch)
    col_pair = lax.ppermute(pair, "cols", PAIRS)
    col_other = lax.ppermute(another, "cols", ODD_PAIRS)

    sent = whole(after_z_kernel, like(SIDE, 8, WIDE), 1 << 22, mine, got)
    arrived = lax.all_to_all(sent, "rows", 0, 0, tiled=True)

    grid_field = like(256, 256)
    outs = (grid_field, grid_field, grid_field, like(9, 16, WIDE))
    scratch = [pltpu.VMEM((6, TALL, WIDE), F32), pltpu.VMEM((3, TALL, WIDE), F32)]
    halos = (row_pair, row_other, col_pair, col_other)
    *bulk, edge = whole(stencil_kernel, outs, 1 << 24, *fields, *halos, scratch=scratch)
    return last_step(arrived, edge, *bulk)


def solution(mesh):
    return jax.shard_map(
        forecast,
        mesh=mesh,
        in_specs=(
            P(None, "rows", "cols", None),
            P(None, "cols"),
            P("rows", "cols"),
            P("rows", "cols"),
            P(),
            P("rows", "cols"),
            P("rows", "cols"),
            P("rows", "cols"),
        ),
        out_specs=(P("rows", "cols"), P("rows", "cols"), P("rows", "cols"), P("rows", "cols")),
        check_vma=False,
    )
```

```python
import math

import jax
import jax.numpy as jnp
from jax import lax
from jax.experimental import pallas as pl
from jax.experimental.pallas import tpu as pltpu
from jax.sharding import PartitionSpec as P


HIGH = lax.Precision.HIGHEST
SIDE = 16
PAIRS = [(i, i ^ 1) for i in range(SIDE)]
ODD_PAIRS = [(i, i + 1) for i in range(1, SIDE - 1, 2)] + [(i + 1, i) for i in range(1, SIDE - 1, 2)]
TIME_OWNERS = [10] + [i for i in range(SIDE) if i != 10]
PAD = 16
TALL = 256 + 2 * PAD
WIDE = 384
VMEM = pl.BlockSpec(memory_space=pltpu.VMEM)
HBM = pl.BlockSpec(memory_space=pltpu.HBM)
F32 = jnp.float32


def like(*shape, dtype=F32):
    return jax.ShapeDtypeStruct(shape, dtype)


def params(limit=48 * 1024 * 1024):
    return pltpu.CompilerParams(vmem_limit_bytes=limit)


def cost(flops, nbytes=1 << 16):
    return pl.CostEstimate(flops=flops, bytes_accessed=nbytes, transcendentals=0)


def swap(x, axis, bits):
    return lax.ppermute(x, axis, [(i, i ^ bits) for i in range(SIDE)])


def row_phase(rows, times, first, quarter):
    freq = first + 4 * (rows // 8) + rows % 4
    return (freq * times + quarter) & 255


def turn(phase):
    return jnp.cos(phase.astype(F32) * (2.0 * math.pi / 256))


def spectrum_kernel(
    chunks, kern_hbm, coef_hbm, cell_hbm, mine_ref, other_ref, data, coef_ref, cell_ref, last, low_hot, sems
):
    wide = 4096 // chunks
    copies = []
    small = [
        pltpu.make_async_copy(coef_hbm, coef_ref, sems.at[chunks]),
        pltpu.make_async_copy(cell_hbm, cell_ref, sems.at[chunks + 1]),
    ]
    for copy in small:
        copy.start()
    for n in range(chunks):
        part = pl.ds(n * wide, wide)
        copies.append(pltpu.make_async_copy(kern_hbm.at[:, :, :, part], data.at[n], sems.at[n]))
        copies[-1].start()
    even = lax.axis_index("cols") % 2 == 0
    first = lax.axis_index("rows") * 16

    rows = lax.broadcasted_iota(jnp.int32, (32, 128), 0)
    lanes = lax.broadcasted_iota(jnp.int32, (32, 128), 1)
    part_of = (rows // 4) % 2
    by_re = turn(row_phase(rows, lanes, first, 64 * part_of))
    by_im = turn(row_phase(rows, lanes, first, 64 * part_of - 64))
    for copy in small:
        copy.wait()
    coef = jnp.concatenate([coef_ref[...]] * 4, axis=0)
    contract = (((1,), (1,)), ((), ()))
    own = (lanes // 32) == (rows % 4)
    from_re = jnp.where(own, lax.dot_general(by_re, coef, contract, precision=HIGH, preferred_element_type=F32), 0.0)
    from_im = jnp.where(own, lax.dot_general(by_im, coef, contract, precision=HIGH, preferred_element_type=F32), 0.0)
    weights = jnp.concatenate([from_re, from_im], axis=1)
    weights = [weights[8 * g : 8 * g + 8].astype(jnp.bfloat16) for g in range(4)]

    cells = cell_ref[...]
    low_of, high_of = cells & 127, cells >> 7
    low_rows = lax.broadcasted_iota(jnp.int32, (128, 512), 0)
    for n in range(8):
        part = slice(n * 512, n * 512 + 512)
        low_hot[:, part] = jnp.where(low_of[:, part] == low_rows, 1.0, 0.0).astype(jnp.bfloat16)

    at_row = lax.broadcasted_iota(jnp.int32, (32, 1), 0)
    pair = [turn(row_phase(at_row, t, first, 64 * ((at_row // 4) % 2))) * (1.0 / 256) for t in (126, 127)]
    for n in range(chunks):
        copies[n].wait()
        got = []
        for g in range(4):
            rhs = jnp.concatenate(
                [data[n, p, 4 * g : 4 * g + 4].reshape(128, wide) for p in range(2)], axis=0
            )
            got.append(jnp.dot(weights[g], rhs, preferred_element_type=F32))
        value = jnp.concatenate(got, axis=0)
        for k in range(2):
            last[k : k + 1, n * wide : n * wide + wide] = jnp.sum(value * pair[k], axis=0, keepdims=True)
        for m in range(wide // 512):
            k = n * (wide // 512) + m
            for half in range(2):
                at = m * 512 + half * 128
                one, two = value[:, at : at + 128], value[:, at + 256 : at + 384]
                mine_ref[k, half * 32 : half * 32 + 32, :] = jnp.where(even, one, two)
                other_ref[k, half * 32 : half * 32 + 32, :] = jnp.where(even, two, one)

    high_rows = lax.broadcasted_iota(jnp.int32, (32, 512), 0)
    placed = jnp.zeros((128, 128), F32)
    for n in range(8):
        part = slice(n * 512, n * 512 + 512)
        here = high_of[:, part] == high_rows
        spread = []
        for k in range(2):
            value = last[k : k + 1, part]
            coarse = value.astype(jnp.bfloat16).astype(F32)
            for piece in (coarse, value - coarse):
                spread.append(jnp.where(here, piece, 0.0).astype(jnp.bfloat16))
        placed = placed + lax.dot_general(
            jnp.concatenate(spread, axis=0), low_hot[:, part], contract, preferred_element_type=F32
        )
    early = placed[0:32] + placed[32:64]
    late = placed[64:96] + placed[96:128]
    index = lax.broadcasted_iota(jnp.int32, (32, 128), 0)
    before = jnp.where(index == 0, 0.0, pltpu.roll(early, 1, 0))
    after = jnp.where(index == 30, 0.0, pltpu.roll(early, 30, 0))
    zeros = jnp.zeros((2, 128), F32)
    for k in range(8):
        tiles = []
        for c in range(2):
            j = 4 * k + 2 * c
            tiles.append(
                jnp.concatenate(
                    [early[j : j + 2], late[j : j + 2], before[j : j + 1], after[j : j + 1], zeros], axis=0
                )
            )
        mine_ref[k, 64:72, :] = jnp.where(even, tiles[0], tiles[1])
        other_ref[k, 64:72, :] = jnp.where(even, tiles[1], tiles[0])


def spectrum(kernel_hat, coefficients, boundary_cell):
    chunks = 8
    wide = 4096 // chunks

    def kernel(*refs):
        spectrum_kernel(chunks, *refs)

    return pl.pallas_call(
        kernel,
        out_shape=(like(8, 72, 128), like(8, 72, 128)),
        in_specs=[HBM, HBM, HBM],
        out_specs=(VMEM, VMEM),
        scratch_shapes=[
            pltpu.VMEM((chunks, 2, 16, 32, wide), jnp.bfloat16),
            pltpu.VMEM((32, 128), F32),
            pltpu.VMEM((1, 4096), jnp.int32),
            pltpu.VMEM((8, 4096), F32),
            pltpu.VMEM((128, 4096), jnp.bfloat16),
            pltpu.SemaphoreType.DMA((chunks + 2,)),
        ],
        compiler_params=params(),
        cost_estimate=cost(1 << 28, 8 << 20),
        name="spectrum",
    )(kernel_hat, *(pltpu.with_memory_space_constraint(v, pltpu.HBM) for v in (coefficients.T, boundary_cell.reshape(1, -1))))


def after_core_kernel(mine, got, keep, one, two, three):
    y = lax.axis_index("cols") // 4
    for out, bits in ((keep, 0), (one, 1), (two, 2), (three, 3)):
        at = pl.ds(2 * (y ^ bits), 2)
        out[...] = mine[at] + got[at]


def after_y_kernel(keep, one, two, three, mine, other):
    total = [keep[i] + one[i] + two[i] + three[i] for i in range(2)]
    low = (lax.axis_index("cols") // 2) % 2 == 0
    mine[...] = jnp.where(low, total[0], total[1])
    other[...] = jnp.where(low, total[1], total[0])


def halves(v):
    coarse = v.astype(jnp.bfloat16).astype(F32)
    return coarse, v - coarse


def after_z_kernel(mine, got, table, sent):
    block = mine[...] + got[...]
    coarse, fine = halves(jnp.concatenate([block[:32], block[32:64]], axis=1))
    spec = jnp.concatenate([coarse, fine, coarse, jnp.zeros_like(fine)], axis=0)
    value = jnp.dot(table[...], spec.astype(jnp.bfloat16), preferred_element_type=F32)
    for n, to in enumerate(TIME_OWNERS):
        sent[n, :, :256] = value[8 * to : 8 * to + 8]
        sent[n, :, 256:] = block[64:]


def whole(kernel, outs, flops, *args, scratch=()):
    return pl.pallas_call(
        kernel,
        out_shape=outs,
        in_specs=[VMEM] * len(args),
        out_specs=jax.tree.map(lambda _: VMEM, outs),
        scratch_shapes=scratch,
        compiler_params=params(),
        cost_estimate=cost(flops),
    )(*args)


def edge_cols_kernel(h, x, y, s, w, pair, other, mat):
    lane = lax.broadcasted_iota(jnp.int32, (64, 128), 1) // 2
    for n in range(4):
        part = slice(64 * n, 64 * n + 64)
        mix = jnp.zeros((64, 128), F32)
        for f, ref in enumerate((h, x, y, s, w)):
            value = ref[part, :].astype(F32)
            first = pltpu.roll(value[:, :128], 2 * f, 1) if f else value[:, :128]
            mix = jnp.where(lane == f, first, mix)
            mix = jnp.where(lane == 8 + f, pltpu.roll(value[:, 128:], 18 + 2 * f, 1), mix)
        mat[part, :] = mix
    even = lax.axis_index("cols") % 2 == 0
    for n in range(2):
        part = slice(128 * n, 128 * n + 128)
        flat = mat[part, :].T
        pair[:, part] = jnp.where(even, flat[16:32], flat[:16])
        other[:, part] = jnp.where(even, flat[:16], flat[16:32])


def sides(axis, pair, other):
    even = lax.axis_index(axis) % 2 == 0
    return jnp.where(even, other, pair), jnp.where(even, pair, other)


def edge_rows_kernel(h, x, y, s, w, col_pair, col_other, pair, other, table):
    left, right = sides("cols", col_pair[...], col_other[...])
    even = lax.axis_index("rows") % 2 == 0
    lane = lax.broadcasted_iota(jnp.int32, (1, 128), 1)
    none = jnp.zeros((1, 128), F32)
    pair[...] = jnp.zeros_like(pair)
    other[...] = jnp.zeros_like(other)
    for f, ref in enumerate((h, x, y, s, w)):
        ends = []
        for at, row in ((0, 0), (254, 255)):
            corner = jnp.where(lane == 0, right[2 * f : 2 * f + 1, row : row + 1], 0.0)
            corner = jnp.where(lane == 127, left[2 * f + 1 : 2 * f + 2, row : row + 1], corner)
            corner = jnp.concatenate([none, corner] if row else [corner, none], axis=0)
            ends.append(jnp.concatenate([ref[at : at + 2, :].astype(F32), corner], axis=1))
        pair[2 * f : 2 * f + 2, :] = jnp.where(even, ends[1], ends[0])
        other[2 * f : 2 * f + 2, :] = jnp.where(even, ends[0], ends[1])
    times = lax.broadcasted_iota(jnp.int32, (128, 128), 0)
    lanes = lax.broadcasted_iota(jnp.int32, (128, 128), 1)
    at_row = lanes % 32
    phase = row_phase(at_row, times, lax.axis_index("rows") * 16, 64 * ((at_row // 4) % 2))
    coarse, fine = halves(turn(phase) * (1.0 / 256))
    table[...] = jnp.where(lanes < 64, coarse, jnp.where(lanes < 96, fine, 0.0)).astype(jnp.bfloat16)


def right_of(v):
    return pltpu.roll(v, WIDE - 1, 1)


def left_of(v):
    return pltpu.roll(v, 1, 1)


def below_of(v):
    return pltpu.roll(v, v.shape[0] - 1, 0)


def above_of(v):
    return pltpu.roll(v, 1, 0)


def fluxes(after, h, q, p, e, c, w):
    opened = 0.5 * (w * after(w))
    damping = 0.5 * opened * (c + after(c))
    mass = opened * (q + after(q)) - damping * (after(h) - h)
    momentum = opened * (e + after(e)) - damping * (after(q) - q)
    shear = -damping * (after(p) - p)
    return mass, momentum, shear


def advance(h, x, y, s, c, w, top, rows):
    e = s * h
    mass_y, momentum_y, shear_y = fluxes(below_of, h, y, x, e, c, w)
    cut = lambda v: v[top : top + rows]
    rise = lambda v: cut(v - above_of(v))
    h, x, y, e, c, w = (cut(v) for v in (h, x, y, e, c, w))
    mass_x, momentum_x, shear_x = fluxes(right_of, h, x, y, e, c, w)
    step = lambda v, a, b: w * (v - 0.25 * ((a - left_of(a)) + rise(b)))
    return step(h, mass_x, mass_y), step(x, momentum_x, shear_y), step(y, shear_x, momentum_y)


def stencil_kernel(h, x, y, s, w, row_pair, row_other, col_pair, col_other, h_out, x_out, y_out, edge, fields, state):
    above, below = sides("rows", row_pair[...], row_other[...])
    left, right = sides("cols", col_pair[...], col_other[...])
    lane = lax.broadcasted_iota(jnp.int32, (256, 128), 1)
    zeros = jnp.zeros((96, 128), F32)
    turned = jnp.concatenate(
        [
            jnp.concatenate([right[:, part], left[:, part], zeros], axis=0).T
            for part in (slice(0, 128), slice(128, 256))
        ],
        axis=0,
    )
    none = jnp.zeros((PAD, WIDE), F32)
    for f, ref in enumerate((h, x, y, s, w)):
        outer = pltpu.roll(turned, (128 - 2 * f) % 128, 1)
        inner = pltpu.roll(turned, 110 - 2 * f, 1)
        fields[f, 0:PAD, :] = none
        fields[f, PAD + 256 :, :] = none
        fields[f, PAD - 2 : PAD, :] = above[2 * f : 2 * f + 2]
        fields[f, PAD + 256 : PAD + 258, :] = below[2 * f : 2 * f + 2]
        fields[f, PAD : PAD + 256, :256] = ref[...].astype(F32)
        fields[f, PAD : PAD + 256, 256:] = jnp.where(lane < 2, outer, jnp.where(lane >= 126, inner, 0.0))
    for n in range(3):
        part = slice(96 * n, 96 * n + 96)
        fields[5, part, :] = jnp.sqrt(fields[3, part, :])

    size = 16
    for at in range(8, TALL - 8, size):
        part = slice(at - 8, at + size + 8)
        got = advance(*(fields[f, part, :] for f in (0, 1, 2, 3, 5, 4)), 8, size)
        for f in range(3):
            state[f, at : at + size, :] = got[f]
    for at in range(PAD, PAD + 256, size):
        part = slice(at - 8, at + size + 8)
        got = advance(*(state[f, part, :] for f in range(3)), *(fields[f, part, :] for f in (3, 5, 4)), 8, size)
        for f, out in enumerate((h_out, x_out, y_out)):
            out[at - PAD : at - PAD + size, :] = got[f][:, :256]
            if at == PAD + 256 - size:
                edge[6 + f, 0:8, :] = got[f][8:]
                edge[6 + f, 8:16, :] = jnp.zeros((8, WIDE), F32)
    for n, f in enumerate((0, 1, 2, 3, 5, 4)):
        edge[n] = fields[f, PAD + 248 : PAD + 264, :]


def last_kernel(arrived, edge, h_in, x_in, y_in, series, h_out, x_out, y_out):
    total = arrived[0]
    for n in range(1, SIDE):
        total = total + arrived[n]
    series[...] = total[:, :256]
    ghost = total[:, 256:]
    at_edge = lax.axis_index("rows") == SIDE - 1
    row = lax.broadcasted_iota(jnp.int32, (16, WIDE), 0)
    lane = lax.broadcasted_iota(jnp.int32, (1, 128), 1)
    first = jnp.concatenate(
        [ghost[0:1], ghost[1:2], jnp.where(lane == 0, ghost[5:6], jnp.where(lane == 127, ghost[4:5], 0.0))], axis=1
    )
    second = jnp.concatenate([ghost[2:3], ghost[3:4], jnp.zeros((1, 128), F32)], axis=1)
    beyond = row == 8
    h, x, y, s, c, w = (edge[n] for n in range(6))
    h, s, c, w = (jnp.where(beyond, fill, v) for v, fill in ((h, first), (s, 1.0), (c, 1.0), (w, 1.0)))
    x, y = (jnp.where(beyond, 0.0, v) for v in (x, y))
    h, x, y = advance(h, x, y, s, c, w, 0, 16)
    h, x, y = jnp.where(beyond, second, h), jnp.where(beyond, 0.0, x), jnp.where(beyond, 0.0, y)
    got = advance(h, x, y, s, c, w, 0, 16)
    redo = jnp.logical_and(at_edge, row[:8, :256] >= 6)
    for f, out in enumerate((h_out, x_out, y_out)):
        out[...] = jnp.where(redo, got[f][:8, :256], edge[6 + f, :8, :256])


def last_step(arrived, edge, height, flux_x, flux_y):
    grid_field = like(256, 256)
    row_block = pl.BlockSpec((8, 256), lambda i: (31, 0))
    return pl.pallas_call(
        last_kernel,
        grid=(1,),
        out_shape=(like(8, 256), grid_field, grid_field, grid_field),
        in_specs=[VMEM, VMEM, HBM, HBM, HBM],
        out_specs=(pl.BlockSpec((8, 256), lambda i: (0, 0)), row_block, row_block, row_block),
        input_output_aliases={2: 1, 3: 2, 4: 3},
        compiler_params=params(),
        cost_estimate=cost(1 << 20),
        name="last",
    )(arrived, edge, height, flux_x, flux_y)


def forecast(
    kernel_hat, coefficients, wave_speed_sq, wet_mask, boundary_cell, height, flux_x, flux_y
):
    fields = (height, flux_x, flux_y, wave_speed_sq, wet_mask)
    mine, other = spectrum(kernel_hat, coefficients, boundary_cell)
    got = swap(other, "cols", 1)

    message = like(16, 256)
    scratch = [pltpu.VMEM((256, 128), F32)]
    pair, another = whole(edge_cols_kernel, (message, message), 1 << 20, *fields, scratch=scratch)
    col_pair = lax.ppermute(pair, "cols", PAIRS)
    col_other = lax.ppermute(another, "cols", ODD_PAIRS)

    slab = like(2, 72, 128)
    keep, one, two, three = whole(after_core_kernel, (slab,) * 4, 1 << 17, mine, got)
    got = [swap(v, "cols", bits) for v, bits in ((two, 8), (one, 4), (three, 12))]

    slab = like(72, 128)
    mine, other = whole(after_y_kernel, (slab, slab), 1 << 17, keep, got[1], got[0], got[2])
    got = swap(other, "cols", 2)

    message = like(16, WIDE)
    outs = (message, message, like(128, 128, dtype=jnp.bfloat16))
    pair, another, table = whole(edge_rows_kernel, outs, 1 << 18, *fields, col_pair, col_other)
    row_pair = lax.ppermute(pair, "rows", PAIRS)
    row_other = lax.ppermute(another, "rows", ODD_PAIRS)

    sent = whole(after_z_kernel, like(SIDE, 8, WIDE), 1 << 22, mine, got, table)
    arrived = lax.all_to_all(sent, "rows", 0, 0, axis_index_groups=[TIME_OWNERS], tiled=True)

    grid_field = like(256, 256)
    outs = (grid_field, grid_field, grid_field, like(9, 16, WIDE))
    scratch = [pltpu.VMEM((6, TALL, WIDE), F32), pltpu.VMEM((3, TALL, WIDE), F32)]
    halos = (row_pair, row_other, col_pair, col_other)
    *bulk, edge = whole(stencil_kernel, outs, 1 << 24, *fields, *halos, scratch=scratch)
    return last_step(arrived, edge, *bulk)


def solution(mesh):
    return jax.shard_map(
        forecast,
        mesh=mesh,
        in_specs=(
            P(None, "rows", "cols", None),
            P(None, "cols"),
            P("rows", "cols"),
            P("rows", "cols"),
            P(),
            P("rows", "cols"),
            P("rows", "cols"),
            P("rows", "cols"),
        ),
        out_specs=(P("rows", "cols"), P("rows", "cols"), P("rows", "cols"), P("rows", "cols")),
        check_vma=False,
    )
```

```python
import math

import jax
import jax.numpy as jnp
from jax import lax
from jax.experimental import pallas as pl
from jax.experimental.pallas import tpu as pltpu
from jax.sharding import PartitionSpec as P


HIGH = lax.Precision.HIGHEST
SIDE = 16
PAIRS = [(i, i ^ 1) for i in range(SIDE)]
ODD_PAIRS = [(i, i + 1) for i in range(1, SIDE - 1, 2)] + [(i + 1, i) for i in range(1, SIDE - 1, 2)]
TIME_OWNERS = [10] + [i for i in range(SIDE) if i != 10]
PAD = 16
TALL = 256 + 2 * PAD
WIDE = 384
VMEM = pl.BlockSpec(memory_space=pltpu.VMEM)
HBM = pl.BlockSpec(memory_space=pltpu.HBM)
F32 = jnp.float32


def like(*shape, dtype=F32):
    return jax.ShapeDtypeStruct(shape, dtype)


def params(limit=48 * 1024 * 1024):
    return pltpu.CompilerParams(vmem_limit_bytes=limit)


def cost(flops, nbytes=1 << 16):
    return pl.CostEstimate(flops=flops, bytes_accessed=nbytes, transcendentals=0)


def swap(x, axis, bits):
    return lax.ppermute(x, axis, [(i, i ^ bits) for i in range(SIDE)])


def row_phase(rows, times, first, quarter):
    freq = first + 4 * (rows // 8) + rows % 4
    return (freq * times + quarter) & 255


def turn(phase):
    return jnp.cos(phase.astype(F32) * (2.0 * math.pi / 256))


def spectrum_kernel(
    chunks, kern_hbm, coef_hbm, cell_hbm, mine_ref, other_ref, data, coef_ref, cell_ref, low_hot, sems
):
    wide = 4096 // chunks
    copies = []
    small = [
        pltpu.make_async_copy(coef_hbm, coef_ref, sems.at[chunks]),
        pltpu.make_async_copy(cell_hbm, cell_ref, sems.at[chunks + 1]),
    ]
    for copy in small:
        copy.start()
    for n in range(chunks):
        part = pl.ds(n * wide, wide)
        copies.append(pltpu.make_async_copy(kern_hbm.at[:, :, :, part], data.at[n], sems.at[n]))
        copies[-1].start()
    even = lax.axis_index("cols") % 2 == 0
    first = lax.axis_index("rows") * 16

    rows = lax.broadcasted_iota(jnp.int32, (32, 128), 0)
    lanes = lax.broadcasted_iota(jnp.int32, (32, 128), 1)
    part_of = (rows // 4) % 2
    by_re = turn(row_phase(rows, lanes, first, 64 * part_of))
    by_im = turn(row_phase(rows, lanes, first, 64 * part_of - 64))
    for copy in small:
        copy.wait()
    coef = jnp.concatenate([coef_ref[...]] * 4, axis=0)
    contract = (((1,), (1,)), ((), ()))
    own = (lanes // 32) == (rows % 4)
    from_re = jnp.where(own, lax.dot_general(by_re, coef, contract, precision=HIGH, preferred_element_type=F32), 0.0)
    from_im = jnp.where(own, lax.dot_general(by_im, coef, contract, precision=HIGH, preferred_element_type=F32), 0.0)
    weights = jnp.concatenate([from_re, from_im], axis=1)
    weights = [weights[8 * g : 8 * g + 8].astype(jnp.bfloat16) for g in range(4)]

    cells = cell_ref[...]
    low_of, high_of = cells & 127, cells >> 7
    low_rows = lax.broadcasted_iota(jnp.int32, (128, 512), 0)
    for n in range(8):
        part = slice(n * 512, n * 512 + 512)
        low_hot[:, part] = jnp.where(low_of[:, part] == low_rows, 1.0, 0.0).astype(jnp.bfloat16)

    at_row = lax.broadcasted_iota(jnp.int32, (32, 1), 0)
    pair = [turn(row_phase(at_row, t, first, 64 * ((at_row // 4) % 2))) * (1.0 / 256) for t in (126, 127)]
    high_rows = lax.broadcasted_iota(jnp.int32, (32, wide), 0)
    placed = jnp.zeros((128, 128), F32)
    for n in range(chunks):
        copies[n].wait()
        got = []
        for g in range(4):
            rhs = jnp.concatenate(
                [data[n, p, 4 * g : 4 * g + 4].reshape(128, wide) for p in range(2)], axis=0
            )
            got.append(jnp.dot(weights[g], rhs, preferred_element_type=F32))
        value = jnp.concatenate(got, axis=0)
        part = slice(n * wide, n * wide + wide)
        here = high_of[:, part] == high_rows
        spread = []
        for k in range(2):
            for piece in halves(jnp.sum(value * pair[k], axis=0, keepdims=True)):
                spread.append(jnp.where(here, piece, 0.0).astype(jnp.bfloat16))
        placed = placed + lax.dot_general(
            jnp.concatenate(spread, axis=0), low_hot[:, part], contract, preferred_element_type=F32
        )
        for m in range(wide // 512):
            k = n * (wide // 512) + m
            for half in range(2):
                at = m * 512 + half * 128
                one, two = value[:, at : at + 128], value[:, at + 256 : at + 384]
                mine_ref[k, half * 32 : half * 32 + 32, :] = jnp.where(even, one, two)
                other_ref[k, half * 32 : half * 32 + 32, :] = jnp.where(even, two, one)

    early = placed[0:32] + placed[32:64]
    late = placed[64:96] + placed[96:128]
    index = lax.broadcasted_iota(jnp.int32, (32, 128), 0)
    before = jnp.where(index == 0, 0.0, pltpu.roll(early, 1, 0))
    after = jnp.where(index == 30, 0.0, pltpu.roll(early, 30, 0))
    zeros = jnp.zeros((2, 128), F32)
    for k in range(8):
        tiles = []
        for c in range(2):
            j = 4 * k + 2 * c
            tiles.append(
                jnp.concatenate(
                    [early[j : j + 2], late[j : j + 2], before[j : j + 1], after[j : j + 1], zeros], axis=0
                )
            )
        mine_ref[k, 64:72, :] = jnp.where(even, tiles[0], tiles[1])
        other_ref[k, 64:72, :] = jnp.where(even, tiles[1], tiles[0])


def spectrum(kernel_hat, coefficients, boundary_cell):
    chunks = 8
    wide = 4096 // chunks

    def kernel(*refs):
        spectrum_kernel(chunks, *refs)

    return pl.pallas_call(
        kernel,
        out_shape=(like(8, 72, 128), like(8, 72, 128)),
        in_specs=[HBM, HBM, HBM],
        out_specs=(VMEM, VMEM),
        scratch_shapes=[
            pltpu.VMEM((chunks, 2, 16, 32, wide), jnp.bfloat16),
            pltpu.VMEM((32, 128), F32),
            pltpu.VMEM((1, 4096), jnp.int32),
            pltpu.VMEM((128, 4096), jnp.bfloat16),
            pltpu.SemaphoreType.DMA((chunks + 2,)),
        ],
        compiler_params=params(),
        cost_estimate=cost(1 << 28, 8 << 20),
        name="spectrum",
    )(kernel_hat, *(pltpu.with_memory_space_constraint(v, pltpu.HBM) for v in (coefficients.T, boundary_cell.reshape(1, -1))))


def after_core_kernel(mine, got, keep, one, two, three):
    y = lax.axis_index("cols") // 4
    for out, bits in ((keep, 0), (one, 1), (two, 2), (three, 3)):
        at = pl.ds(2 * (y ^ bits), 2)
        out[...] = mine[at] + got[at]


def after_y_kernel(keep, one, two, three, mine, other):
    total = [keep[i] + one[i] + two[i] + three[i] for i in range(2)]
    low = (lax.axis_index("cols") // 2) % 2 == 0
    mine[...] = jnp.where(low, total[0], total[1])
    other[...] = jnp.where(low, total[1], total[0])


def halves(v):
    coarse = v.astype(jnp.bfloat16).astype(F32)
    return coarse, v - coarse


def after_z_kernel(mine, got, table, sent):
    block = mine[...] + got[...]
    coarse, fine = halves(jnp.concatenate([block[:32], block[32:64]], axis=1))
    spec = jnp.concatenate([coarse, fine, coarse, jnp.zeros_like(fine)], axis=0)
    value = jnp.dot(table[...], spec.astype(jnp.bfloat16), preferred_element_type=F32)
    for n, to in enumerate(TIME_OWNERS):
        sent[n, :, :256] = value[8 * to : 8 * to + 8]
        sent[n, :, 256:] = block[64:]


def whole(kernel, outs, flops, *args, scratch=()):
    return pl.pallas_call(
        kernel,
        out_shape=outs,
        in_specs=[VMEM] * len(args),
        out_specs=jax.tree.map(lambda _: VMEM, outs),
        scratch_shapes=scratch,
        compiler_params=params(),
        cost_estimate=cost(flops),
    )(*args)


def edge_cols_kernel(h, x, y, s, w, pair, other, mat):
    lane = lax.broadcasted_iota(jnp.int32, (64, 128), 1) // 2
    for n in range(4):
        part = slice(64 * n, 64 * n + 64)
        mix = jnp.zeros((64, 128), F32)
        for f, ref in enumerate((h, x, y, s, w)):
            value = ref[part, :].astype(F32)
            first = pltpu.roll(value[:, :128], 2 * f, 1) if f else value[:, :128]
            mix = jnp.where(lane == f, first, mix)
            mix = jnp.where(lane == 8 + f, pltpu.roll(value[:, 128:], 18 + 2 * f, 1), mix)
        mat[part, :] = mix
    even = lax.axis_index("cols") % 2 == 0
    for n in range(2):
        part = slice(128 * n, 128 * n + 128)
        flat = mat[part, :].T
        pair[:, part] = jnp.where(even, flat[16:32], flat[:16])
        other[:, part] = jnp.where(even, flat[:16], flat[16:32])


def sides(axis, pair, other):
    even = lax.axis_index(axis) % 2 == 0
    return jnp.where(even, other, pair), jnp.where(even, pair, other)


def edge_rows_kernel(h, x, y, s, w, col_pair, col_other, pair, other, table):
    left, right = sides("cols", col_pair[...], col_other[...])
    even = lax.axis_index("rows") % 2 == 0
    lane = lax.broadcasted_iota(jnp.int32, (1, 128), 1)
    none = jnp.zeros((1, 128), F32)
    pair[...] = jnp.zeros_like(pair)
    other[...] = jnp.zeros_like(other)
    for f, ref in enumerate((h, x, y, s, w)):
        ends = []
        for at, row in ((0, 0), (254, 255)):
            corner = jnp.where(lane == 0, right[2 * f : 2 * f + 1, row : row + 1], 0.0)
            corner = jnp.where(lane == 127, left[2 * f + 1 : 2 * f + 2, row : row + 1], corner)
            corner = jnp.concatenate([none, corner] if row else [corner, none], axis=0)
            ends.append(jnp.concatenate([ref[at : at + 2, :].astype(F32), corner], axis=1))
        pair[2 * f : 2 * f + 2, :] = jnp.where(even, ends[1], ends[0])
        other[2 * f : 2 * f + 2, :] = jnp.where(even, ends[0], ends[1])
    times = lax.broadcasted_iota(jnp.int32, (128, 128), 0)
    lanes = lax.broadcasted_iota(jnp.int32, (128, 128), 1)
    at_row = lanes % 32
    phase = row_phase(at_row, times, lax.axis_index("rows") * 16, 64 * ((at_row // 4) % 2))
    coarse, fine = halves(turn(phase) * (1.0 / 256))
    table[...] = jnp.where(lanes < 64, coarse, jnp.where(lanes < 96, fine, 0.0)).astype(jnp.bfloat16)


def right_of(v):
    return pltpu.roll(v, WIDE - 1, 1)


def left_of(v):
    return pltpu.roll(v, 1, 1)


def below_of(v):
    return pltpu.roll(v, v.shape[0] - 1, 0)


def above_of(v):
    return pltpu.roll(v, 1, 0)


def faces(after, c, w):
    opened = 0.5 * (w * after(w))
    return opened, 0.5 * opened * (c + after(c))


def fluxes(after, opened, damping, h, q, p, e):
    mass = opened * (q + after(q)) - damping * (after(h) - h)
    momentum = opened * (e + after(e)) - damping * (after(q) - q)
    shear = damping * (p - after(p))
    return mass, momentum, shear


def advance(h, x, y, s, w, by_x, by_y, top, rows):
    e = s * h
    mass_y, momentum_y, shear_y = fluxes(below_of, *by_y, h, y, x, e)
    cut = lambda v: v[top : top + rows]
    rise = lambda v: cut(v - above_of(v))
    h, x, y, e = (cut(v) for v in (h, x, y, e))
    mass_x, momentum_x, shear_x = fluxes(right_of, *by_x, h, x, y, e)
    step = lambda v, a, b: w * (v - 0.25 * ((a - left_of(a)) + rise(b)))
    return step(h, mass_x, mass_y), step(x, momentum_x, shear_y), step(y, shear_x, momentum_y)


def stencil_kernel(h, x, y, s, w, row_pair, row_other, col_pair, col_other, h_out, x_out, y_out, edge, fields, state, kept):
    above, below = sides("rows", row_pair[...], row_other[...])
    left, right = sides("cols", col_pair[...], col_other[...])
    lane = lax.broadcasted_iota(jnp.int32, (256, 128), 1)
    zeros = jnp.zeros((96, 128), F32)
    turned = jnp.concatenate(
        [
            jnp.concatenate([right[:, part], left[:, part], zeros], axis=0).T
            for part in (slice(0, 128), slice(128, 256))
        ],
        axis=0,
    )
    none = jnp.zeros((PAD, WIDE), F32)
    for f, ref in enumerate((h, x, y, s, w)):
        outer = pltpu.roll(turned, (128 - 2 * f) % 128, 1)
        inner = pltpu.roll(turned, 110 - 2 * f, 1)
        fields[f, 0:PAD, :] = none
        fields[f, PAD + 256 :, :] = none
        fields[f, PAD - 2 : PAD, :] = above[2 * f : 2 * f + 2]
        fields[f, PAD + 256 : PAD + 258, :] = below[2 * f : 2 * f + 2]
        fields[f, PAD : PAD + 256, :256] = ref[...].astype(F32)
        fields[f, PAD : PAD + 256, 256:] = jnp.where(lane < 2, outer, jnp.where(lane >= 126, inner, 0.0))
    for n in range(3):
        part = slice(96 * n, 96 * n + 96)
        fields[5, part, :] = jnp.sqrt(fields[3, part, :])

    size = 64
    for at in range(8, TALL - 8, size):
        rows = min(size, TALL - 8 - at)
        part, own = slice(at - 8, at + rows + 8), slice(at, at + rows)
        by_x = faces(right_of, fields[5, own, :], fields[4, own, :])
        by_y = faces(below_of, fields[5, part, :], fields[4, part, :])
        got = advance(*(fields[f, part, :] for f in range(4)), fields[4, own, :], by_x, by_y, 8, rows)
        for f in range(3):
            state[f, own, :] = got[f]
        for f, v in enumerate((*by_x, *(v[8 : 8 + rows] for v in by_y))):
            kept[f, own, :] = v
    for at in range(PAD, PAD + 256, size):
        part, own = slice(at - 8, at + size + 8), slice(at, at + size)
        by_x = (kept[0, own, :], kept[1, own, :])
        by_y = (kept[2, part, :], kept[3, part, :])
        got = advance(*(state[f, part, :] for f in range(3)), fields[3, part, :], fields[4, own, :], by_x, by_y, 8, size)
        for f, out in enumerate((h_out, x_out, y_out)):
            out[at - PAD : at - PAD + size, :] = got[f][:, :256]
            if at == PAD + 256 - size:
                edge[6 + f, 0:8, :] = got[f][size - 8 :]
                edge[6 + f, 8:16, :] = jnp.zeros((8, WIDE), F32)
    for n, f in enumerate((0, 1, 2, 3, 5, 4)):
        edge[n] = fields[f, PAD + 248 : PAD + 264, :]


def last_kernel(arrived, edge, h_in, x_in, y_in, series, h_out, x_out, y_out):
    total = arrived[0]
    for n in range(1, SIDE):
        total = total + arrived[n]
    series[...] = total[:, :256]
    ghost = total[:, 256:]
    at_edge = lax.axis_index("rows") == SIDE - 1
    row = lax.broadcasted_iota(jnp.int32, (16, WIDE), 0)
    lane = lax.broadcasted_iota(jnp.int32, (1, 128), 1)
    first = jnp.concatenate(
        [ghost[0:1], ghost[1:2], jnp.where(lane == 0, ghost[5:6], jnp.where(lane == 127, ghost[4:5], 0.0))], axis=1
    )
    second = jnp.concatenate([ghost[2:3], ghost[3:4], jnp.zeros((1, 128), F32)], axis=1)
    beyond = row == 8
    h, x, y, s, c, w = (edge[n] for n in range(6))
    h, s, c, w = (jnp.where(beyond, fill, v) for v, fill in ((h, first), (s, 1.0), (c, 1.0), (w, 1.0)))
    x, y = (jnp.where(beyond, 0.0, v) for v in (x, y))
    by_x, by_y = faces(right_of, c, w), faces(below_of, c, w)
    h, x, y = advance(h, x, y, s, w, by_x, by_y, 0, 16)
    h, x, y = jnp.where(beyond, second, h), jnp.where(beyond, 0.0, x), jnp.where(beyond, 0.0, y)
    got = advance(h, x, y, s, w, by_x, by_y, 0, 16)
    redo = jnp.logical_and(at_edge, row[:8, :256] >= 6)
    for f, out in enumerate((h_out, x_out, y_out)):
        out[...] = jnp.where(redo, got[f][:8, :256], edge[6 + f, :8, :256])


def last_step(arrived, edge, height, flux_x, flux_y):
    grid_field = like(256, 256)
    row_block = pl.BlockSpec((8, 256), lambda i: (31, 0))
    return pl.pallas_call(
        last_kernel,
        grid=(1,),
        out_shape=(like(8, 256), grid_field, grid_field, grid_field),
        in_specs=[VMEM, VMEM, HBM, HBM, HBM],
        out_specs=(pl.BlockSpec((8, 256), lambda i: (0, 0)), row_block, row_block, row_block),
        input_output_aliases={2: 1, 3: 2, 4: 3},
        compiler_params=params(),
        cost_estimate=cost(1 << 20),
        name="last",
    )(arrived, edge, height, flux_x, flux_y)


def forecast(
    kernel_hat, coefficients, wave_speed_sq, wet_mask, boundary_cell, height, flux_x, flux_y
):
    fields = (height, flux_x, flux_y, wave_speed_sq, wet_mask)
    mine, other = spectrum(kernel_hat, coefficients, boundary_cell)
    got = swap(other, "cols", 1)

    message = like(16, 256)
    scratch = [pltpu.VMEM((256, 128), F32)]
    pair, another = whole(edge_cols_kernel, (message, message), 1 << 20, *fields, scratch=scratch)
    col_pair = lax.ppermute(pair, "cols", PAIRS)
    col_other = lax.ppermute(another, "cols", ODD_PAIRS)

    slab = like(2, 72, 128)
    keep, one, two, three = whole(after_core_kernel, (slab,) * 4, 1 << 17, mine, got)
    got = [swap(v, "cols", bits) for v, bits in ((two, 8), (one, 4), (three, 12))]

    slab = like(72, 128)
    mine, other = whole(after_y_kernel, (slab, slab), 1 << 17, keep, got[1], got[0], got[2])
    got = swap(other, "cols", 2)

    message = like(16, WIDE)
    outs = (message, message, like(128, 128, dtype=jnp.bfloat16))
    pair, another, table = whole(edge_rows_kernel, outs, 1 << 18, *fields, col_pair, col_other)
    row_pair = lax.ppermute(pair, "rows", PAIRS)
    row_other = lax.ppermute(another, "rows", ODD_PAIRS)

    sent = whole(after_z_kernel, like(SIDE, 8, WIDE), 1 << 22, mine, got, table)
    arrived = lax.all_to_all(sent, "rows", 0, 0, axis_index_groups=[TIME_OWNERS], tiled=True)

    grid_field = like(256, 256)
    outs = (grid_field, grid_field, grid_field, like(9, 16, WIDE))
    scratch = [pltpu.VMEM((n, TALL, WIDE), F32) for n in (6, 3, 4)]
    halos = (row_pair, row_other, col_pair, col_other)
    *bulk, edge = whole(stencil_kernel, outs, 1 << 24, *fields, *halos, scratch=scratch)
    return last_step(arrived, edge, *bulk)


def solution(mesh):
    return jax.shard_map(
        forecast,
        mesh=mesh,
        in_specs=(
            P(None, "rows", "cols", None),
            P(None, "cols"),
            P("rows", "cols"),
            P("rows", "cols"),
            P(),
            P("rows", "cols"),
            P("rows", "cols"),
            P("rows", "cols"),
        ),
        out_specs=(P("rows", "cols"), P("rows", "cols"), P("rows", "cols"), P("rows", "cols")),
        check_vma=False,
    )
```

```python
import math

import jax
import jax.numpy as jnp
from jax import lax
from jax.experimental import pallas as pl
from jax.experimental.pallas import tpu as pltpu
from jax.sharding import PartitionSpec as P


HIGH = lax.Precision.HIGHEST
SIDE = 16
PAIRS = [(i, i ^ 1) for i in range(SIDE)]
ODD_PAIRS = [(i, i + 1) for i in range(1, SIDE - 1, 2)] + [(i + 1, i) for i in range(1, SIDE - 1, 2)]
TIME_OWNERS = [10] + [i for i in range(SIDE) if i != 10]
PAD = 16
TALL = 256 + 2 * PAD
WIDE = 384
VMEM = pl.BlockSpec(memory_space=pltpu.VMEM)
HBM = pl.BlockSpec(memory_space=pltpu.HBM)
F32 = jnp.float32


def like(*shape, dtype=F32):
    return jax.ShapeDtypeStruct(shape, dtype)


def params(limit=48 * 1024 * 1024):
    return pltpu.CompilerParams(vmem_limit_bytes=limit)


def cost(flops, nbytes=1 << 16):
    return pl.CostEstimate(flops=flops, bytes_accessed=nbytes, transcendentals=0)


def swap(x, axis, bits):
    return lax.ppermute(x, axis, [(i, i ^ bits) for i in range(SIDE)])


def row_phase(rows, times, first, quarter):
    freq = first + 4 * (rows // 8) + rows % 4
    return (freq * times + quarter) & 255


def turn(phase):
    return jnp.cos(phase.astype(F32) * (2.0 * math.pi / 256))


def spectrum_kernel(
    chunks, kern_hbm, coef_hbm, cell_hbm, mine_ref, other_ref, data, coef_ref, cell_ref, low_hot, sems
):
    wide = 4096 // chunks
    copies = []
    small = [
        pltpu.make_async_copy(coef_hbm, coef_ref, sems.at[chunks]),
        pltpu.make_async_copy(cell_hbm, cell_ref, sems.at[chunks + 1]),
    ]
    for copy in small:
        copy.start()
    for n in range(chunks):
        part = pl.ds(n * wide, wide)
        copies.append(pltpu.make_async_copy(kern_hbm.at[:, :, :, part], data.at[n], sems.at[n]))
        copies[-1].start()
    even = lax.axis_index("cols") % 2 == 0
    first = lax.axis_index("rows") * 16

    rows = lax.broadcasted_iota(jnp.int32, (32, 128), 0)
    lanes = lax.broadcasted_iota(jnp.int32, (32, 128), 1)
    part_of = (rows // 4) % 2
    by_re = turn(row_phase(rows, lanes, first, 64 * part_of))
    by_im = turn(row_phase(rows, lanes, first, 64 * part_of - 64))
    for copy in small:
        copy.wait()
    coef = jnp.concatenate([coef_ref[...]] * 4, axis=0)
    contract = (((1,), (1,)), ((), ()))
    own = (lanes // 32) == (rows % 4)
    from_re = jnp.where(own, lax.dot_general(by_re, coef, contract, precision=HIGH, preferred_element_type=F32), 0.0)
    from_im = jnp.where(own, lax.dot_general(by_im, coef, contract, precision=HIGH, preferred_element_type=F32), 0.0)
    weights = jnp.concatenate([from_re, from_im], axis=1)
    weights = [weights[8 * g : 8 * g + 8].astype(jnp.bfloat16) for g in range(4)]

    cells = cell_ref[...]
    low_of, high_of = cells & 127, cells >> 7
    low_rows = lax.broadcasted_iota(jnp.int32, (128, 512), 0)
    for n in range(8):
        part = slice(n * 512, n * 512 + 512)
        low_hot[:, part] = jnp.where(low_of[:, part] == low_rows, 1.0, 0.0).astype(jnp.bfloat16)

    at_row = lax.broadcasted_iota(jnp.int32, (32, 1), 0)
    pair = [turn(row_phase(at_row, t, first, 64 * ((at_row // 4) % 2))) * (1.0 / 256) for t in (126, 127)]
    high_rows = lax.broadcasted_iota(jnp.int32, (32, wide), 0)
    placed = jnp.zeros((128, 128), F32)
    for n in range(chunks):
        copies[n].wait()
        got = []
        for g in range(4):
            rhs = jnp.concatenate(
                [data[n, p, 4 * g : 4 * g + 4].reshape(128, wide) for p in range(2)], axis=0
            )
            got.append(jnp.dot(weights[g], rhs, preferred_element_type=F32))
        value = jnp.concatenate(got, axis=0)
        part = slice(n * wide, n * wide + wide)
        here = high_of[:, part] == high_rows
        spread = []
        for k in range(2):
            for piece in halves(jnp.sum(value * pair[k], axis=0, keepdims=True)):
                spread.append(jnp.where(here, piece, 0.0).astype(jnp.bfloat16))
        placed = placed + lax.dot_general(
            jnp.concatenate(spread, axis=0), low_hot[:, part], contract, preferred_element_type=F32
        )
        for m in range(wide // 512):
            k = n * (wide // 512) + m
            for half in range(2):
                at = m * 512 + half * 128
                one, two = value[:, at : at + 128], value[:, at + 256 : at + 384]
                mine_ref[k, half * 32 : half * 32 + 32, :] = jnp.where(even, one, two)
                other_ref[k, half * 32 : half * 32 + 32, :] = jnp.where(even, two, one)

    early = placed[0:32] + placed[32:64]
    late = placed[64:96] + placed[96:128]
    index = lax.broadcasted_iota(jnp.int32, (32, 128), 0)
    before = jnp.where(index == 0, 0.0, pltpu.roll(early, 1, 0))
    after = jnp.where(index == 30, 0.0, pltpu.roll(early, 30, 0))
    zeros = jnp.zeros((2, 128), F32)
    for k in range(8):
        tiles = []
        for c in range(2):
            j = 4 * k + 2 * c
            tiles.append(
                jnp.concatenate(
                    [early[j : j + 2], late[j : j + 2], before[j : j + 1], after[j : j + 1], zeros], axis=0
                )
            )
        mine_ref[k, 64:72, :] = jnp.where(even, tiles[0], tiles[1])
        other_ref[k, 64:72, :] = jnp.where(even, tiles[1], tiles[0])


def spectrum(kernel_hat, coefficients, boundary_cell):
    chunks = 8
    wide = 4096 // chunks

    def kernel(*refs):
        spectrum_kernel(chunks, *refs)

    return pl.pallas_call(
        kernel,
        out_shape=(like(8, 72, 128), like(8, 72, 128)),
        in_specs=[HBM, HBM, HBM],
        out_specs=(VMEM, VMEM),
        scratch_shapes=[
            pltpu.VMEM((chunks, 2, 16, 32, wide), jnp.bfloat16),
            pltpu.VMEM((32, 128), F32),
            pltpu.VMEM((1, 4096), jnp.int32),
            pltpu.VMEM((128, 4096), jnp.bfloat16),
            pltpu.SemaphoreType.DMA((chunks + 2,)),
        ],
        compiler_params=params(),
        cost_estimate=cost(1 << 28, 8 << 20),
        name="spectrum",
    )(kernel_hat, *(pltpu.with_memory_space_constraint(v, pltpu.HBM) for v in (coefficients.T, boundary_cell.reshape(1, -1))))


def after_core_kernel(mine, got, keep, one, two, three):
    y = lax.axis_index("cols") // 4
    for out, bits in ((keep, 0), (one, 1), (two, 2), (three, 3)):
        at = pl.ds(2 * (y ^ bits), 2)
        out[...] = mine[at] + got[at]


def after_y_kernel(keep, one, two, three, mine, other):
    total = [keep[i] + one[i] + two[i] + three[i] for i in range(2)]
    low = (lax.axis_index("cols") // 2) % 2 == 0
    mine[...] = jnp.where(low, total[0], total[1])
    other[...] = jnp.where(low, total[1], total[0])


def halves(v):
    coarse = v.astype(jnp.bfloat16).astype(F32)
    return coarse, v - coarse


def after_z_kernel(mine, got, table, sent):
    block = mine[...] + got[...]
    coarse, fine = halves(jnp.concatenate([block[:32], block[32:64]], axis=1))
    spec = jnp.concatenate([coarse, fine, coarse, jnp.zeros_like(fine)], axis=0)
    value = jnp.dot(table[...], spec.astype(jnp.bfloat16), preferred_element_type=F32)
    for n, to in enumerate(TIME_OWNERS):
        sent[n, :, :256] = value[8 * to : 8 * to + 8]
        sent[n, :, 256:] = block[64:]


def whole(kernel, outs, flops, *args, scratch=()):
    return pl.pallas_call(
        kernel,
        out_shape=outs,
        in_specs=[VMEM] * len(args),
        out_specs=jax.tree.map(lambda _: VMEM, outs),
        scratch_shapes=scratch,
        compiler_params=params(),
        cost_estimate=cost(flops),
    )(*args)


def edge_cols_kernel(h, x, y, s, w, pair, other, mat):
    lane = lax.broadcasted_iota(jnp.int32, (64, 128), 1) // 2
    for n in range(4):
        part = slice(64 * n, 64 * n + 64)
        mix = jnp.zeros((64, 128), F32)
        for f, ref in enumerate((h, x, y, s, w)):
            value = ref[part, :].astype(F32)
            first = pltpu.roll(value[:, :128], 2 * f, 1) if f else value[:, :128]
            mix = jnp.where(lane == f, first, mix)
            mix = jnp.where(lane == 8 + f, pltpu.roll(value[:, 128:], 18 + 2 * f, 1), mix)
        mat[part, :] = mix
    even = lax.axis_index("cols") % 2 == 0
    for n in range(2):
        part = slice(128 * n, 128 * n + 128)
        flat = mat[part, :].T
        pair[:, part] = jnp.where(even, flat[16:32], flat[:16])
        other[:, part] = jnp.where(even, flat[:16], flat[16:32])


def sides(axis, pair, other):
    even = lax.axis_index(axis) % 2 == 0
    return jnp.where(even, other, pair), jnp.where(even, pair, other)


def edge_rows_kernel(h, x, y, s, w, col_pair, col_other, pair, other, table):
    left, right = sides("cols", col_pair[...], col_other[...])
    even = lax.axis_index("rows") % 2 == 0
    lane = lax.broadcasted_iota(jnp.int32, (1, 128), 1)
    none = jnp.zeros((1, 128), F32)
    pair[...] = jnp.zeros_like(pair)
    other[...] = jnp.zeros_like(other)
    for f, ref in enumerate((h, x, y, s, w)):
        ends = []
        for at, row in ((0, 0), (254, 255)):
            corner = jnp.where(lane == 0, right[2 * f : 2 * f + 1, row : row + 1], 0.0)
            corner = jnp.where(lane == 127, left[2 * f + 1 : 2 * f + 2, row : row + 1], corner)
            corner = jnp.concatenate([none, corner] if row else [corner, none], axis=0)
            ends.append(jnp.concatenate([ref[at : at + 2, :].astype(F32), corner], axis=1))
        pair[2 * f : 2 * f + 2, :] = jnp.where(even, ends[1], ends[0])
        other[2 * f : 2 * f + 2, :] = jnp.where(even, ends[0], ends[1])
    times = lax.broadcasted_iota(jnp.int32, (128, 128), 0)
    lanes = lax.broadcasted_iota(jnp.int32, (128, 128), 1)
    at_row = lanes % 32
    phase = row_phase(at_row, times, lax.axis_index("rows") * 16, 64 * ((at_row // 4) % 2))
    coarse, fine = halves(turn(phase) * (1.0 / 256))
    table[...] = jnp.where(lanes < 64, coarse, jnp.where(lanes < 96, fine, 0.0)).astype(jnp.bfloat16)


def right_of(v):
    return pltpu.roll(v, WIDE - 1, 1)


def left_of(v):
    return pltpu.roll(v, 1, 1)


def below_of(v):
    return pltpu.roll(v, v.shape[0] - 1, 0)


def above_of(v):
    return pltpu.roll(v, 1, 0)


def faces(after, c, w):
    opened = 0.5 * (w * after(w))
    return opened, 0.5 * opened * (c + after(c))


def fluxes(after, opened, damping, h, q, p, e):
    mass = opened * (q + after(q)) - damping * (after(h) - h)
    momentum = opened * (e + after(e)) - damping * (after(q) - q)
    shear = damping * (p - after(p))
    return mass, momentum, shear


def advance(h, x, y, s, w, by_x, by_y, top, rows):
    e = s * h
    mass_y, momentum_y, shear_y = fluxes(below_of, *by_y, h, y, x, e)
    cut = lambda v: v[top : top + rows]
    rise = lambda v: cut(v - above_of(v))
    h, x, y, e = (cut(v) for v in (h, x, y, e))
    mass_x, momentum_x, shear_x = fluxes(right_of, *by_x, h, x, y, e)
    step = lambda v, a, b: w * (v - 0.25 * ((a - left_of(a)) + rise(b)))
    return step(h, mass_x, mass_y), step(x, momentum_x, shear_y), step(y, shear_x, momentum_y)


def stencil_kernel(h, x, y, s, w, row_pair, row_other, col_pair, col_other, h_out, x_out, y_out, edge, fields, state, kept):
    above, below = sides("rows", row_pair[...], row_other[...])
    left, right = sides("cols", col_pair[...], col_other[...])
    lane = lax.broadcasted_iota(jnp.int32, (256, 128), 1)
    zeros = jnp.zeros((96, 128), F32)
    turned = jnp.concatenate(
        [
            jnp.concatenate([right[:, part], left[:, part], zeros], axis=0).T
            for part in (slice(0, 128), slice(128, 256))
        ],
        axis=0,
    )
    none = jnp.zeros((PAD, WIDE), F32)
    for f, ref in enumerate((h, x, y, s, w)):
        outer = pltpu.roll(turned, (128 - 2 * f) % 128, 1)
        inner = pltpu.roll(turned, 110 - 2 * f, 1)
        fields[f, 0:PAD, :] = none
        fields[f, PAD + 256 :, :] = none
        fields[f, PAD - 2 : PAD, :] = above[2 * f : 2 * f + 2]
        fields[f, PAD + 256 : PAD + 258, :] = below[2 * f : 2 * f + 2]
        fields[f, PAD : PAD + 256, :256] = ref[...].astype(F32)
        fields[f, PAD : PAD + 256, 256:] = jnp.where(lane < 2, outer, jnp.where(lane >= 126, inner, 0.0))
    for n in range(3):
        part = slice(96 * n, 96 * n + 96)
        fields[5, part, :] = jnp.sqrt(fields[3, part, :])

    size = 64
    for at in range(8, TALL - 8, size):
        rows = min(size, TALL - 8 - at)
        part, own = slice(at - 8, at + rows + 8), slice(at, at + rows)
        by_x = faces(right_of, fields[5, own, :], fields[4, own, :])
        by_y = faces(below_of, fields[5, part, :], fields[4, part, :])
        got = advance(*(fields[f, part, :] for f in range(4)), fields[4, own, :], by_x, by_y, 8, rows)
        for f in range(3):
            state[f, own, :] = got[f]
        for f, v in enumerate((*by_x, *(v[8 : 8 + rows] for v in by_y))):
            kept[f, own, :] = v
    for at in range(PAD, PAD + 256, size):
        part, own = slice(at - 8, at + size + 8), slice(at, at + size)
        by_x = (kept[0, own, :], kept[1, own, :])
        by_y = (kept[2, part, :], kept[3, part, :])
        got = advance(*(state[f, part, :] for f in range(3)), fields[3, part, :], fields[4, own, :], by_x, by_y, 8, size)
        for f, out in enumerate((h_out, x_out, y_out)):
            out[at - PAD : at - PAD + size, :] = got[f][:, :256]
            if at == PAD + 256 - size:
                edge[6 + f, 0:8, :] = got[f][size - 8 :]
                edge[6 + f, 8:16, :] = jnp.zeros((8, WIDE), F32)
    for n, f in enumerate((0, 1, 2, 3, 5, 4)):
        edge[n] = fields[f, PAD + 248 : PAD + 264, :]


def last_kernel(arrived, edge, h_in, x_in, y_in, series, h_out, x_out, y_out, block, sems):
    total = arrived[0]
    for n in range(1, SIDE):
        total = total + arrived[n]
    series[...] = total[:, :256]
    ghost = total[:, 256:]

    @pl.when(lax.axis_index("rows") == SIDE - 1)
    def _():
        row = lax.broadcasted_iota(jnp.int32, (16, WIDE), 0)
        lane = lax.broadcasted_iota(jnp.int32, (1, 128), 1)
        first = jnp.concatenate(
            [ghost[0:1], ghost[1:2], jnp.where(lane == 0, ghost[5:6], jnp.where(lane == 127, ghost[4:5], 0.0))], axis=1
        )
        second = jnp.concatenate([ghost[2:3], ghost[3:4], jnp.zeros((1, 128), F32)], axis=1)
        beyond = row == 8
        h, x, y, s, c, w = (edge[n] for n in range(6))
        h, s, c, w = (jnp.where(beyond, fill, v) for v, fill in ((h, first), (s, 1.0), (c, 1.0), (w, 1.0)))
        x, y = (jnp.where(beyond, 0.0, v) for v in (x, y))
        by_x, by_y = faces(right_of, c, w), faces(below_of, c, w)
        h, x, y = advance(h, x, y, s, w, by_x, by_y, 0, 16)
        h, x, y = jnp.where(beyond, second, h), jnp.where(beyond, 0.0, x), jnp.where(beyond, 0.0, y)
        got = advance(h, x, y, s, w, by_x, by_y, 0, 16)
        redo = row[:8, :256] >= 6
        copies = []
        for f, out in enumerate((h_out, x_out, y_out)):
            block[f] = jnp.where(redo, got[f][:8, :256], edge[6 + f, :8, :256])
            copies.append(pltpu.make_async_copy(block.at[f], out.at[pl.ds(248, 8), :], sems.at[f]))
            copies[-1].start()
        for copy in copies:
            copy.wait()


def last_step(arrived, edge, height, flux_x, flux_y):
    grid_field = like(256, 256)
    return pl.pallas_call(
        last_kernel,
        out_shape=(like(8, 256), grid_field, grid_field, grid_field),
        in_specs=[VMEM, VMEM, HBM, HBM, HBM],
        out_specs=(VMEM, HBM, HBM, HBM),
        scratch_shapes=[pltpu.VMEM((3, 8, 256), F32), pltpu.SemaphoreType.DMA((3,))],
        input_output_aliases={2: 1, 3: 2, 4: 3},
        compiler_params=params(),
        cost_estimate=cost(1 << 20),
        name="last",
    )(arrived, edge, height, flux_x, flux_y)


def forecast(
    kernel_hat, coefficients, wave_speed_sq, wet_mask, boundary_cell, height, flux_x, flux_y
):
    fields = (height, flux_x, flux_y, wave_speed_sq, wet_mask)
    mine, other = spectrum(kernel_hat, coefficients, boundary_cell)
    got = swap(other, "cols", 1)

    message = like(16, 256)
    scratch = [pltpu.VMEM((256, 128), F32)]
    pair, another = whole(edge_cols_kernel, (message, message), 1 << 20, *fields, scratch=scratch)
    col_pair = lax.ppermute(pair, "cols", PAIRS)
    col_other = lax.ppermute(another, "cols", ODD_PAIRS)

    slab = like(2, 72, 128)
    keep, one, two, three = whole(after_core_kernel, (slab,) * 4, 1 << 17, mine, got)
    got = [swap(v, "cols", bits) for v, bits in ((two, 8), (one, 4), (three, 12))]

    slab = like(72, 128)
    mine, other = whole(after_y_kernel, (slab, slab), 1 << 17, keep, got[1], got[0], got[2])
    got = swap(other, "cols", 2)

    message = like(16, WIDE)
    outs = (message, message, like(128, 128, dtype=jnp.bfloat16))
    pair, another, table = whole(edge_rows_kernel, outs, 1 << 18, *fields, col_pair, col_other)
    row_pair = lax.ppermute(pair, "rows", PAIRS)
    row_other = lax.ppermute(another, "rows", ODD_PAIRS)

    sent = whole(after_z_kernel, like(SIDE, 8, WIDE), 1 << 22, mine, got, table)
    arrived = lax.all_to_all(sent, "rows", 0, 0, axis_index_groups=[TIME_OWNERS], tiled=True)

    grid_field = like(256, 256)
    outs = (grid_field, grid_field, grid_field, like(9, 16, WIDE))
    scratch = [pltpu.VMEM((n, TALL, WIDE), F32) for n in (6, 3, 4)]
    halos = (row_pair, row_other, col_pair, col_other)
    *bulk, edge = whole(stencil_kernel, outs, 1 << 24, *fields, *halos, scratch=scratch)
    return last_step(arrived, edge, *bulk)


def solution(mesh):
    return jax.shard_map(
        forecast,
        mesh=mesh,
        in_specs=(
            P(None, "rows", "cols", None),
            P(None, "cols"),
            P("rows", "cols"),
            P("rows", "cols"),
            P(),
            P("rows", "cols"),
            P("rows", "cols"),
            P("rows", "cols"),
        ),
        out_specs=(P("rows", "cols"), P("rows", "cols"), P("rows", "cols"), P("rows", "cols")),
        check_vma=False,
    )
```
